128 devices in a mesh: front: 4 (over x_lo, core), row: 4 (over z), col: 8 (over y, x_hi).
Axes of the slice: x: 4 (x_hi: 2, x_lo: 2; x = x_hi * 2 + x_lo), y: 4, z: 4, core: 2. Of those that a mesh axis runs over, the one named last changes fastest.
Arguments:
- front_entries: float32 [4, 8192, 8192], P('front', 'row', 'col'), may hold values from -12 to 128, as said below
- kid_u: bfloat16 [16, 4096, 128], P('front', ('row', 'col')), may hold values from -0.7109375 to 0.7109375
- kid_v: bfloat16 [16, 4096, 128], P('front', ('row', 'col')), may hold values from -0.7109375 to 0.7109375
- kid_d: bfloat16 [16, 4096, 256], P('front', ('row', 'col')), may hold values from -2.09375 to 2.09375
- kid_counts: int32 [16], replicated, may hold values from 32 to 128
- kid_blocks: int32 [16, 16], replicated, may hold values from 0 to 31, as said below
Outputs:
- front_out: float32 [4, 8192, 8192], P('front', 'row', 'col')
The draws below stay inside these ranges and needn't reach their ends.
Inputs may be any that keep to these rules, and one draw needn't show every extreme that they name: `front_entries`: diagonal entries lie between 64 and 128; the other entries are of order one. `kid_blocks`: each row holds distinct block positions in increasing order. `kid_counts`: rank columns at or beyond a child's count are padding.
All inputs are finite; a program needn't handle non-finite values.
Results may differ from the reference program's by a relative error of at most 0.004.
Values may be sent and summed in bfloat16 or wider, within the bound.
No kernel may reach another device: no remote copies, remote signals or barrier semaphores. Data moves between devices by JAX's collectives and lax.ppermute only.
A program may use at most 128 MiB of HBM per device.

```python
import jax
import jax.numpy as jnp
from jax import lax

NF = 8192
NC = 4096
R = 128
LEAF = 256
PANEL = 256
PANELS = 4
KIDS = 4
FRONTS = 4
KIDS_ALL = 16
N_FRONT = 4


def draw_front_entries(key, part):
    spread_key, diagonal_key = jax.random.split(jax.random.fold_in(key, 11))
    spread = jnp.clip(jax.random.normal(spread_key, (FRONTS, NF, NF), jnp.float32), -6.0, 6.0)
    twisted = spread - jnp.swapaxes(spread, 1, 2)
    diagonal_values = jax.random.uniform(diagonal_key, (FRONTS, NF), jnp.float32, 64.0, 128.0)
    places = jnp.arange(NF)
    return twisted.at[:, places, places].set(diagonal_values)


def draw_kid_blocks(key, part):
    child_keys = jax.random.split(jax.random.fold_in(key, 23), KIDS_ALL)

    def single(child_key):
        return jnp.sort(jax.random.permutation(child_key, NF // LEAF)[:NC // LEAF]).astype(jnp.int32)
    return jax.vmap(single)(child_keys)


def place_ends(drawn, rng, least, top_value):
    longest = drawn.shape.index(max(drawn.shape))
    spots = []
    for shift in (0, 1):
        where = [jax.random.randint(jax.random.fold_in(rng, axis), (), 0, length) for axis, length in enumerate(drawn.shape)]
        where[longest] = (where[longest] + shift) % drawn.shape[longest]
        spots.append(tuple(where))
    return drawn.at[spots[0]].set(least).at[spots[1]].set(top_value)


def shard_levels(own_key, dims, pieces, low, largest):
    def one(dim, blocks):
        draws = jax.random.uniform(jax.random.fold_in(jax.random.fold_in(own_key, 6), dim), (blocks,), jnp.float32, low / len(pieces), largest / len(pieces))
        return jnp.repeat(jnp.exp(draws), dims[dim] // blocks).reshape((-1,) + (1,) * (len(dims) - dim - 1))

    level = one(*pieces[0])
    for cut in pieces[1:]:
        level = level * one(*cut)
    return level


def noise(own_key, dims, deviation, bound, cuts=(), kind=jnp.bfloat16):
    entries = deviation * jax.random.normal(own_key, dims, jnp.float32)
    if cuts:
        entries = entries * shard_levels(own_key, dims, cuts, -0.22, 0.18)
    return jnp.clip(entries, -bound, bound).astype(kind)


def setup_inputs(seed: int = 0) -> dict:
    key_of = jax.random.split(jax.random.key(seed), 7)
    return {
        "front_entries": draw_front_entries(jax.random.fold_in(key_of[6], 71), 0),
        "kid_u": noise(key_of[1], (KIDS_ALL, NC, R), (0.4 * R ** -0.25), 0.7109375, ((0, 4), (1, 32))),
        "kid_v": noise(key_of[2], (KIDS_ALL, NC, R), (0.4 * R ** -0.25), 0.7109375, ((0, 4), (1, 32))),
        "kid_d": noise(key_of[3], (KIDS_ALL, NC, LEAF), 0.35, 2.09375, ((0, 4), (1, 32))),
        "kid_counts": place_ends(jax.random.randint(key_of[4], (KIDS_ALL,), R // 4, R + 1), jax.random.fold_in(key_of[4], 1), R // 4, R).astype(jnp.int32),
        "kid_blocks": draw_kid_blocks(jax.random.fold_in(key_of[6], 71), 0),
    }


def assemble(front, children_u, children_v, children_d, counts, blocks):
    leaves = NC // LEAF
    identity = jnp.eye(leaves, dtype=jnp.float32)
    for child in range(KIDS):
        column_mask = (jnp.arange(R, dtype=jnp.int32) < counts[child]).astype(jnp.float32)
        factor_u = children_u[child].astype(jnp.float32) * column_mask[None, :]
        lowrank = jnp.dot(factor_u, children_v[child].astype(jnp.float32).T, precision=lax.Precision.HIGHEST)
        diagonal_blocks = children_d[child].astype(jnp.float32).reshape(leaves, LEAF, LEAF)
        update = lowrank.reshape(leaves, LEAF, leaves, LEAF) + diagonal_blocks[:, :, None, :] * identity[:, None, :, None]
        places = (blocks[child][:, None] * LEAF + jnp.arange(LEAF, dtype=jnp.int32)[None, :]).reshape(-1).astype(jnp.int32)
        front = front.at[places[:, None], places[None, :]].add(update.reshape(NC, NC))
    return front

def factor(front):
    for panel_index in range(PANELS):
        start = panel_index * PANEL
        finish = start + PANEL
        pivot = front[start:finish, start:finish]
        inverse = jnp.linalg.solve(pivot, jnp.eye(PANEL, dtype=jnp.float32))
        lower = jnp.dot(front[finish:, start:finish], inverse, precision=lax.Precision.HIGHEST)
        lower_half = lax.optimization_barrier(lower.astype(jnp.bfloat16)).astype(jnp.float32)
        upper_half = lax.optimization_barrier(front[start:finish, finish:].astype(jnp.bfloat16)).astype(jnp.float32)
        front = front.at[finish:, finish:].add(-jnp.dot(lower_half, upper_half, precision=lax.Precision.HIGHEST))
        front = front.at[finish:, start:finish].set(lower)
    return front

def reference(front_entries, kid_u, kid_v, kid_d, kid_counts, kid_blocks):

    def one_front(parent):
        first_child = ((parent + N_FRONT - 1) % N_FRONT * KIDS).astype(jnp.int32)

        def choose_rows(array):
            return lax.dynamic_slice_in_dim(array, first_child, KIDS, 0)
        front = lax.dynamic_index_in_dim(front_entries, parent, 0, keepdims=False)
        front = assemble(front, choose_rows(kid_u), choose_rows(kid_v), choose_rows(kid_d), choose_rows(kid_counts), choose_rows(kid_blocks))
        return factor(front)
    return lax.map(one_front, jnp.arange(FRONTS, dtype=jnp.int32))
```

```python
import jax
import jax.numpy as jnp
from jax import lax
from jax.experimental import pallas as pl
from jax.experimental.pallas import tpu as pltpu
from jax.sharding import Mesh
from jax.sharding import PartitionSpec as P

PANEL = 256
PANELS = 4
K = PANEL * PANELS
COL = ("col_0", "col_1")
ROW_COL = ("row", "col_0", "col_1")
F32 = jnp.float32
BF16 = jnp.bfloat16


def dot(a, b):
    return jnp.dot(a, b, preferred_element_type=F32)


def split(a):
    high = a.astype(BF16)
    return high, (a - high.astype(F32)).astype(BF16)


def dot3(a, b):
    a_high, a_low = split(a)
    b_high, b_low = split(b)
    return dot(a_high, b_high) + (dot(a_high, b_low) + dot(a_low, b_high))


def total(flags, values):
    out = None
    for flag, value in zip(flags, values):
        piece = jnp.where(flag, value, jnp.zeros_like(value))
        out = piece if out is None else out + piece
    return out


def assemble_kernel(scal, front, u, v, d, out, out_b):
    step = pl.program_id(0)
    low = lax.dot_general(u[...], v[...], (((1,), (1,)), ((), ())), preferred_element_type=F32)
    out[...] = front[...] + low
    place = step - 4 * scal[1]
    for block in range(4):
        @pl.when((scal[0] == 1) & (place == block))
        def _(block=block):
            cols = slice(block * PANEL, (block + 1) * PANEL)
            out[:, cols] = out[:, cols] + d[block]
    out_b[...] = out[...].astype(BF16)


def assemble(scal, front, u, v, d):
    rows, cols = front.shape
    rank = u.shape[1]
    return pl.pallas_call(
        assemble_kernel,
        name="assemble",
        out_shape=(jax.ShapeDtypeStruct((rows, cols), F32), jax.ShapeDtypeStruct((rows, cols), BF16)),
        grid_spec=pltpu.PrefetchScalarGridSpec(
            num_scalar_prefetch=1,
            grid=(rows // PANEL,),
            in_specs=[
                pl.BlockSpec((PANEL, cols), lambda i, s: (i, 0)),
                pl.BlockSpec((PANEL, rank), lambda i, s: (i, 0)),
                pl.BlockSpec((cols, rank), lambda i, s: (0, 0)),
                pl.BlockSpec((4, PANEL, PANEL), lambda i, s: (0, 0, 0)),
            ],
            out_specs=(
                pl.BlockSpec((PANEL, cols), lambda i, s: (i, 0)),
                pl.BlockSpec((PANEL, cols), lambda i, s: (i, 0)),
            ),
        ),
        cost_estimate=pl.CostEstimate(
            flops=2 * rows * cols * rank, bytes_accessed=10 * rows * cols, transcendentals=0
        ),
    )(scal, front, u, v, d)


def invert_into(inv, index, pivot):
    eye = lax.broadcasted_iota(jnp.int32, (PANEL, PANEL), 0) == lax.broadcasted_iota(
        jnp.int32, (PANEL, PANEL), 1
    )
    one = jnp.where(eye, 1.0, 0.0)
    diagonal = jnp.where(eye, pivot, 0.0)
    down = 1.0 / jnp.sum(diagonal, axis=1, keepdims=True)
    across = 1.0 / jnp.sum(diagonal, axis=0, keepdims=True)
    rest = jnp.where(eye, 0.0, -pivot * across)
    power = rest.astype(BF16)
    series = one + rest
    for _ in range(4):
        power = dot(power, power).astype(BF16)
        series = series + dot(series.astype(BF16), power)
    inv[index] = series * down
    p_high, p_low = split(pivot)

    def improve():
        x = inv[index]
        x_high, x_low = split(x)
        error = one - (dot(p_high, x_high) + (dot(p_high, x_low) + dot(p_low, x_high)))
        inv[index] = x + dot(x_high, error.astype(BF16))
        return jnp.max(jnp.abs(error))

    size = improve()

    @pl.when(jnp.logical_not(size < 0.25))
    def _():
        norm = jnp.max(jnp.sum(jnp.abs(pivot), axis=0)) * jnp.max(jnp.sum(jnp.abs(pivot), axis=1))
        inv[index] = pivot.T * (1.0 / norm)

    def more(carry):
        trips, last = carry
        return trips + 1, improve()

    lax.while_loop(
        lambda carry: (carry[0] < 100) & jnp.logical_not(carry[1] < 4e-3), more, (jnp.int32(0), size)
    )


def factor_kernel(scal, tile, *refs):
    chunks = refs[:8]
    kc, g0, g1, g2, g3, a, c, inv = refs[8:]
    outs = (g0, g1, g2, g3)

    @pl.when(scal[0] == 1)
    def _():
        c[...] = tile[...]

        @pl.when(scal[1] == 1)
        def _():
            a[...] = tile[...]

        @pl.when(scal[1] == 0)
        def _():
            for t in range(8):
                start = pl.multiple_of(scal[2 + t] * 128, 128)
                a[pl.ds(start, 128), :] = chunks[t][...].astype(F32)

        for k in range(PANELS):
            s, e = k * PANEL, (k + 1) * PANEL
            invert_into(inv, k, a[s:e, s:e])
            if e < K:
                lower = dot3(a[e:, s:e], inv[k])
                a[e:, s:e] = lower
                lower_b = lower.astype(BF16)
                a[e:, e:] = a[e:, e:] - dot(lower_b, a[s:e, e:].astype(BF16))
                c[e:, :] = c[e:, :] - dot(lower_b, c[s:e, :].astype(BF16))

        @pl.when(scal[1] == 1)
        def _():
            kc[...] = a[...]
            rows = lax.broadcasted_iota(jnp.int32, (K, K), 0)
            cols = lax.broadcasted_iota(jnp.int32, (K, K), 1)
            c[...] = jnp.where(rows == cols, 1.0, 0.0)

        @pl.when(scal[1] == 0)
        def _():
            kc[...] = c[...]

        for k in reversed(range(PANELS)):
            s, e = k * PANEL, (k + 1) * PANEL
            part = dot3(inv[k], c[s:e, :])
            part_b = part.astype(BF16)
            for q in range(4):
                outs[q][s:e, :] = part_b[:, q * PANEL : (q + 1) * PANEL]
            if k:
                c[:s, :] = c[:s, :] - dot(a[:s, s:e].astype(BF16), part_b)


def factor(scal, tile, chunks):
    quarter = jax.ShapeDtypeStruct((K, PANEL), BF16)
    return pl.pallas_call(
        factor_kernel,
        name="factor",
        out_shape=(jax.ShapeDtypeStruct((K, K), F32),) + (quarter,) * 4,
        grid_spec=pltpu.PrefetchScalarGridSpec(
            num_scalar_prefetch=1,
            grid=(1,),
            in_specs=[pl.BlockSpec((K, K), lambda i, s: (0, 0))]
            + [pl.BlockSpec((128, K), lambda i, s: (0, 0))] * 8,
            out_specs=(pl.BlockSpec((K, K), lambda i, s: (0, 0)),)
            + (pl.BlockSpec((K, PANEL), lambda i, s: (0, 0)),) * 4,
            scratch_shapes=[
                pltpu.VMEM((K, K), F32),
                pltpu.VMEM((K, K), F32),
                pltpu.VMEM((PANELS, PANEL, PANEL), F32),
            ],
        ),
        compiler_params=pltpu.CompilerParams(vmem_limit_bytes=56 * 1024 * 1024),
        cost_estimate=pl.CostEstimate(flops=10 * K * K * K, bytes_accessed=12 * K * K, transcendentals=0),
    )(scal, tile, *chunks)


def trail_kernel(scal, tile, left, kc, g0, g1, g2, g3, out):
    block = scal[2 + pl.program_id(0)]
    keep = (scal[0] == 1) & (block < 8)

    @pl.when(keep)
    def _():
        out[...] = kc[...]

    @pl.when(jnp.logical_not(keep))
    def _():
        for q, g in enumerate((g0, g1, g2, g3)):
            cols = slice(q * PANEL, (q + 1) * PANEL)
            product = dot(left[0], g[...])
            out[:, cols] = jnp.where(scal[1] == 1, product, tile[:, cols] - product)


def trail(scal, tile, left, kc, gs):
    rows, cols = tile.shape
    whole = pl.BlockSpec((K, PANEL), lambda i, s: (0, 0))
    return pl.pallas_call(
        trail_kernel,
        name="trail",
        out_shape=jax.ShapeDtypeStruct((rows, cols), F32),
        grid_spec=pltpu.PrefetchScalarGridSpec(
            num_scalar_prefetch=1,
            grid=(16,),
            in_specs=[
                pl.BlockSpec((128, cols), lambda i, s: (s[2 + i], 0)),
                pl.BlockSpec((1, 128, K), lambda i, s: (i, 0, 0)),
                pl.BlockSpec((128, cols), lambda i, s: (jnp.minimum(s[2 + i], 7), 0)),
                whole, whole, whole, whole,
            ],
            out_specs=pl.BlockSpec((128, cols), lambda i, s: (s[2 + i], 0)),
        ),
        cost_estimate=pl.CostEstimate(
            flops=2 * rows * cols * K, bytes_accessed=10 * rows * cols, transcendentals=0
        ),
    )(scal, tile, left, kc, *gs)


STEPS = [(dy, dx) for dy in range(4) for dx in range(2)]


def col_pairs(dy, dx):
    return [
        (2 * y + h, 2 * ((y + dy) % 4) + (h ^ dx)) for y in range(4) for h in range(2)
    ]


def gather_col(value):
    return [
        value if step == (0, 0) else lax.ppermute(value, COL, col_pairs(*step)) for step in STEPS
    ]


def scatter_col(pieces, place):
    got = [pieces[0]] + [lax.ppermute(pieces[i], COL, [(0, i)]) for i in range(1, 8)]
    return total([place == i for i in range(8)], got)


def local(front_entries, kid_u, kid_v, kid_d, kid_counts, kid_blocks):
    children, _, rank = kid_u.shape
    f = lax.axis_index("front")
    r = lax.axis_index("row")
    y = lax.axis_index("col_0")
    h = lax.axis_index("col_1")
    place = 2 * y + h
    first_child = (f + 3) % 4 * children
    counts = lax.dynamic_slice_in_dim(kid_counts, first_child, children, 0)
    blocks = lax.dynamic_slice_in_dim(kid_blocks, first_child, children, 0)
    by_source = blocks.reshape(children, 4, 4)

    pack = jnp.concatenate((kid_v, kid_d), axis=2)
    got_u, got_p = [], []
    for k in range(4):
        pairs = [(i * 4 + j, (i + 1) % 4 * 4 + (j + k) % 4) for i in range(4) for j in range(4)]
        got_u.append(lax.ppermute(kid_u, ("front", "row"), pairs))
        one = lax.dynamic_index_in_dim(pack, (r + k) % 4, 0, keepdims=False)
        got_p.append(lax.ppermute(one, ("front", "row"), pairs))

    here = jnp.sum(
        jnp.where(jnp.arange(4, dtype=jnp.int32) == y, by_source, 0), axis=2
    )
    sources = [(r - k) % 4 for k in range(4)]
    came = [
        jnp.sum(jnp.where(jnp.arange(4, dtype=jnp.int32) == s, here, 0), axis=1) for s in sources
    ]

    slots = []
    for window in range(2):
        flags = [(b // 4 == 2 * r + window)[:, None, None] for b in came]
        slots.append(total(flags, got_u))
    rank_mask = (jnp.arange(rank, dtype=jnp.int32)[None, :] < counts[:, None])[:, None, :]
    slot_u = jnp.where(rank_mask[None], jnp.stack(slots), jnp.zeros((), BF16))
    all_u = gather_col(slot_u)

    mine = jnp.arange(children, dtype=jnp.int32) == r
    came_r = [jnp.sum(jnp.where(mine, b, 0)) for b in came]
    windows = jnp.arange(8, dtype=jnp.int32)
    send = total([(b // 4 == windows)[:, None, None] for b in came_r], [g[None] for g in got_p])
    back = lax.all_to_all(send, COL, 0, 0)

    def positions(window):
        inside = by_source // 4 == window
        return jnp.sum(jnp.where(inside, by_source - 4 * window, 0), axis=1)

    spots = jnp.arange(4, dtype=jnp.int32)
    pos_r = jnp.sum(jnp.where(mine[:, None], positions(place), 0), axis=0)
    back = back.reshape(4, 2, 128, -1)
    placed = total(
        [(pos_r[q] == spots)[:, None, None, None] for q in range(4)], [back[q][None] for q in range(4)]
    )
    placed = placed.reshape(K, -1)
    v_mine = placed[:, :rank]
    d_mine = placed[:, rank:]
    v_got = [v_mine] + [
        lax.ppermute(v_mine, "row", [(i, (i + s) % 4) for i in range(4)]) for s in range(1, 4)
    ]
    d_sum = d_mine.astype(F32)
    for s in range(1, 4):
        pairs = [
            (((t - s) % 4) * 8 + 2 * t + x, t * 8 + 2 * t + x) for t in range(4) for x in range(2)
        ]
        d_sum = d_sum + lax.ppermute(d_mine, ROW_COL, pairs).astype(F32)
    d_tile = d_sum.reshape(4, PANEL, PANEL)

    v_all = jnp.concatenate(
        [total([sources[s] == kid for s in range(4)], v_got) for kid in range(children)], axis=1
    )
    spot_u = [positions(2 * r + window) for window in range(2)]
    halves = []
    for dx in range(2):
        parts = []
        for window in range(2):
            flags, values = [], []
            for dy in range(4):
                q = (y - dy) % 4
                at = jnp.sum(jnp.where(spots == q, spot_u[window], 0), axis=1)
                flags.append((at[None, :] == spots[:, None])[:, :, None, None])
                values.append(all_u[2 * dy + dx][window][None])
            parts.append(total(flags, values))
        halves.append(jnp.concatenate(parts, axis=0))
    even = jnp.where(h == 0, halves[0], halves[1])
    odd = jnp.where(h == 0, halves[1], halves[0])
    u_all = jnp.stack((even, odd), axis=1)
    u_all = u_all.transpose(0, 1, 3, 2, 4).reshape(8 * PANEL, children * rank)

    flag = lambda value: value.astype(jnp.int32)
    tile, tile_b = assemble(
        jnp.stack([flag(r == y), h]).astype(jnp.int32), front_entries[0], u_all, v_all, d_tile
    )

    pieces = [tile_b[i * 128 : (i + 1) * 128] for i in range(16)]
    top = gather_col(scatter_col(pieces[:8], place))
    low = gather_col(scatter_col(pieces[8:], place))
    order = jnp.stack([2 * ((y - dy) % 4) + (h ^ dx) for dy, dx in STEPS]).astype(jnp.int32)

    scal = jnp.concatenate((jnp.stack([flag(r == 0), flag(place == 0)]), order)).astype(jnp.int32)
    kc, *g = factor(scal, tile, top)

    def up(value, hops):
        return lax.ppermute(value, "row", [(i, i + 1) for i in range(hops)])

    def down(value, hops):
        return lax.ppermute(value, "row", [(-i % 4, -(i + 1) % 4) for i in range(hops)])

    root = r == 0
    up1, down1 = up(g[0], 1), down(g[3], 1)
    up2, down2 = up(jnp.where(root, g[1], up1), 2), down(jnp.where(root, g[2], down1), 2)
    up3, down3 = up(jnp.where(root, g[2], up2), 3), down(jnp.where(root, g[1], down2), 3)
    rows_are = [r == i for i in range(4)]
    quarters = [
        total(rows_are, (g[0], up1, up2, up3)),
        total(rows_are, (g[1], up2, up3, down3)),
        total(rows_are, (g[2], up3, down3, down2)),
        total(rows_are, (g[3], down3, down2, down1)),
    ]
    scal = jnp.concatenate((scal[:2], order, order + 8))
    return trail(scal, tile, jnp.stack(top + low), kc, quarters)[None]


def solution(mesh):
    finer = Mesh(
        mesh.devices.reshape(mesh.shape["front"], mesh.shape["row"], 4, 2),
        ("front", "row", "col_0", "col_1"),
    )
    in_specs = (
        P("front", "row", COL),
        P("front", ROW_COL, None),
        P("front", ROW_COL, None),
        P("front", ROW_COL, None),
        P(),
        P(),
    )
    out_specs = P("front", "row", COL)
    return jax.shard_map(local, mesh=finer, in_specs=in_specs, out_specs=out_specs, check_vma=False)
```

```python
import jax
import jax.numpy as jnp
from jax import lax
from jax.experimental import pallas as pl
from jax.experimental.pallas import tpu as pltpu
from jax.sharding import Mesh
from jax.sharding import PartitionSpec as P


PANEL = 256
PANELS = 4
K = PANEL * PANELS
COL = ("col_0", "col_1")
ROW_COL = ("row", "col_0", "col_1")
F32 = jnp.float32
BF16 = jnp.bfloat16


def dot(a, b):
    return jnp.dot(a, b, preferred_element_type=F32)


def split(a):
    high = a.astype(BF16)
    return high, (a - high.astype(F32)).astype(BF16)


def total(flags, values):
    out = None
    for flag, value in zip(flags, values):
        piece = jnp.where(flag, value, jnp.zeros_like(value))
        out = piece if out is None else out + piece
    return out


SHIFT = 96.0


def identity():
    rows = lax.broadcasted_iota(jnp.int32, (PANEL, PANEL), 0)
    return rows == lax.broadcasted_iota(jnp.int32, (PANEL, PANEL), 1)


def invert_into(inv, index, pivot):
    eye = identity()
    one = jnp.where(eye, 1.0, 0.0)
    diagonal = jnp.where(eye, pivot, 0.0)
    down = 1.0 / jnp.sum(diagonal, axis=1, keepdims=True)
    across = 1.0 / jnp.sum(diagonal, axis=0, keepdims=True)
    rest = jnp.where(eye, 0.0, -pivot * across)
    power = rest.astype(BF16)
    series = one + rest
    for _ in range(3):
        power = dot(power, power).astype(BF16)
        series = series + dot(series.astype(BF16), power)
    inv[index] = series * down
    p_high, p_low = split(pivot)

    def improve():
        x = inv[index]
        x_high, x_low = split(x)
        error = one - (dot(p_high, x_high) + (dot(p_high, x_low) + dot(p_low, x_high)))
        inv[index] = x + dot(x_high, error.astype(BF16))
        square = error * error
        return jnp.max(jnp.sum(square, axis=0)) * jnp.max(jnp.sum(square, axis=1))

    size = improve()

    @pl.when(jnp.logical_not(size < 0.5))
    def _():
        norm = jnp.max(jnp.sum(jnp.abs(pivot), axis=0)) * jnp.max(jnp.sum(jnp.abs(pivot), axis=1))
        inv[index] = pivot.T * (1.0 / norm)

    def more(carry):
        trips, _ = carry
        return trips + 1, improve()

    lax.while_loop(
        lambda carry: (carry[0] < 100) & jnp.logical_not(carry[1] < 4e-6), more, (jnp.int32(0), size)
    )


def factor_kernel(scal, tile, top, kc, g0, g1, g2, g3, a, c, inv):
    outs = (g0, g1, g2, g3)
    row, place = scal[0], scal[3]

    @pl.when(row == 0)
    def _():
        a[...] = top[...].astype(F32)
        for k in range(PANELS):
            s, e = k * PANEL, (k + 1) * PANEL
            a[s:e, s:e] = a[s:e, s:e] + jnp.where(identity(), SHIFT, 0.0)

        @pl.when(place == 0)
        def _():
            c[...] = a[...]

        @pl.when(place != 0)
        def _():
            c[...] = tile[...]

        for k in range(PANELS):
            s, e = k * PANEL, (k + 1) * PANEL
            invert_into(inv, k, a[s:e, s:e])
            if e < K:
                lower = dot(a[e:, s:e].astype(BF16), inv[k].astype(BF16))
                a[e:, s:e] = lower
                lower_b = lower.astype(BF16)
                a[e:, e:] = a[e:, e:] - dot(lower_b, a[s:e, e:].astype(BF16))
                c[e:, :] = c[e:, :] - dot(lower_b, c[s:e, :].astype(BF16))

        @pl.when(place == 0)
        def _():
            kc[...] = a[...]
            rows = lax.broadcasted_iota(jnp.int32, (K, K), 0)
            cols = lax.broadcasted_iota(jnp.int32, (K, K), 1)
            c[...] = jnp.where(rows == cols, 1.0, 0.0)

        @pl.when(place != 0)
        def _():
            kc[...] = c[...]

        for k in reversed(range(PANELS)):
            s, e = k * PANEL, (k + 1) * PANEL
            part = dot(inv[k].astype(BF16), c[s:e, :].astype(BF16))
            part_b = part.astype(BF16)
            for q in range(4):
                outs[q][s:e, :] = part_b[:, q * PANEL : (q + 1) * PANEL]
            if k:
                c[:s, :] = c[:s, :] - dot(a[:s, s:e].astype(BF16), part_b)


def whole(shape):
    return pl.BlockSpec(shape, lambda i, s: (0,) * len(shape))


def call(kernel, scal, args, in_specs, outs, out_specs, grid=(1,), scratch=(), flops=0):
    moved = sum(x.size * x.dtype.itemsize for x in args)
    single = not isinstance(outs, tuple)
    return pl.pallas_call(
        kernel,
        out_shape=outs,
        grid_spec=pltpu.PrefetchScalarGridSpec(
            num_scalar_prefetch=1,
            grid=grid,
            in_specs=in_specs,
            out_specs=out_specs if single else tuple(out_specs),
            scratch_shapes=list(scratch),
        ),
        compiler_params=pltpu.CompilerParams(vmem_limit_bytes=56 * 1024 * 1024),
        cost_estimate=pl.CostEstimate(flops=flops, bytes_accessed=2 * moved, transcendentals=0),
    )(scal, *args)


def simple(kernel, scal, args, outs, scratch=(), flops=0):
    return call(
        kernel, scal, args, [whole(x.shape) for x in args], tuple(outs),
        [whole(x.shape) for x in outs], scratch=scratch, flops=flops,
    )


def shape(*dims, dtype=BF16):
    return jax.ShapeDtypeStruct(dims, dtype)


def factor(scal, tile, top):
    return call(
        factor_kernel, scal, [tile, top],
        [whole((K, K)), whole((K, K))],
        (shape(K, K, dtype=F32),) + (shape(K, PANEL),) * 4,
        [whole((K, K))] + [whole((K, PANEL))] * 4,
        scratch=[pltpu.VMEM((K, K), F32), pltpu.VMEM((K, K), F32), pltpu.VMEM((PANELS, PANEL, PANEL), F32)],
        flops=10 * K * K * K,
    )


COUNT_AT, BLOCK_AT = 4, 8


def block_of(scal, kid, source_row, q):
    return scal[BLOCK_AT + kid * 16 + source_row * 4 + q]


def spot(scal, kid, window, q):
    at = jnp.int32(-1)
    for source_row in range(4):
        block = block_of(scal, kid, source_row, q)
        at = jnp.where((block >> 2) == window, block & 3, at)
    return at


def chosen(flags, values):
    acc = None
    for flag, value in zip(flags, values):
        value = value.astype(F32)
        value = jnp.where(flag, value, jnp.zeros_like(value))
        acc = value if acc is None else acc + value
    return acc


def halve_kernel(scal, front, *outs):
    for i, out in enumerate(outs):
        out[...] = front[i * PANEL : (i + 1) * PANEL, :].astype(BF16)


def halve(scal, front, part):
    return call(
        halve_kernel, scal, [front], [pl.BlockSpec((K, K), lambda i, s: (part, 0))],
        (shape(PANEL, K),) * 4, [whole((PANEL, K))] * 4,
    )


def pick_left_kernel(scal, u0, u1, u2, u3, out):
    row, y = scal[0], scal[1]
    lane = lax.broadcasted_iota(jnp.int32, (128, 128), 1)
    for kid in range(4):
        live = lane < scal[COUNT_AT + kid]
        blocks = [block_of(scal, kid, (row - k) & 3, y) for k in range(4)]
        for window in range(2):
            flags = [(b >> 2) == 2 * row + window for b in blocks]
            value = chosen(flags, [u[kid] for u in (u0, u1, u2, u3)])
            value = jnp.where(live, value, 0.0).astype(BF16)
            for peer in range(8):
                out[peer, window, kid] = value


def pick_right_kernel(scal, p0, p1, p2, p3, out):
    row, y = scal[0], scal[1]
    blocks = [block_of(scal, row, (row - k) & 3, y) for k in range(4)]
    rights = [p[...] for p in (p0, p1, p2, p3)]
    first = chosen([(b >> 2) == 0 for b in blocks], rights).astype(BF16)
    for peer in range(8):
        out[peer, :, :128] = chosen([(b >> 2) == peer for b in blocks], rights).astype(BF16)
        out[peer, :, 128:] = first


def pick_blocks_kernel(scal, d0, d1, d2, d3, out):
    row, y = scal[0], scal[1]
    for window in range(8):
        flags, values = [], []
        for kid in range(4):
            for k, d in enumerate((d0, d1, d2, d3)):
                flags.append(block_of(scal, kid, (row - k) & 3, y) == 4 * window + row)
                values.append(d[kid])
        out[window] = chosen(flags, values).astype(BF16)


def place_right_kernel(scal, back, out_own, out_first):
    row, place = scal[0], scal[3]
    own = [spot(scal, row, place, q) for q in range(4)]
    first = [spot(scal, row, 0, q) for q in range(4)]
    for at in range(4):
        for half in range(2):
            rows = slice((2 * at + half) * 128, (2 * at + half + 1) * 128)
            for spots, out, cols in ((own, out_own, slice(0, 128)), (first, out_first, slice(128, 256))):
                flags = [spots[q] == at for q in range(4)]
                out[rows, :] = chosen(flags, [back[2 * q + half, :, cols] for q in range(4)]).astype(BF16)


def place_blocks_kernel(scal, back, out):
    for half in range(2):
        acc = back[half].astype(F32)
        for q in range(1, 4):
            acc = acc + back[2 * q + half].astype(F32)
        out[half * 128 : (half + 1) * 128, :] = acc.astype(BF16)


def slab_kernel(scal, near, far, us, *refs, part):
    vs, ks = refs[:4], refs[4:-4]
    out, left, right, acc = refs[-4:]
    row, y, h, place = scal[0], scal[1], scal[2], scal[3]
    for s in range(4):
        kid = (row - s) & 3
        right[:, s * 128 : (s + 1) * 128] = vs[s][...]
        hits = [spot(scal, kid, 2 * row + part, q) == y for q in range(4)]
        value = chosen(hits, [us[2 * q + h, part, kid] for q in range(4)])
        left[:, s * 128 : (s + 1) * 128] = value.astype(BF16)
    raw = jnp.where(h == 0, near[:128, :].astype(F32), far[...].astype(F32))
    acc[...] = raw + lax.dot_general(
        left[...], right[...], (((1,), (1,)), ((), ())), preferred_element_type=F32
    )
    if ks:
        @pl.when(row == 0)
        def _():
            extra = ks[0][...].astype(F32) + ks[1][...].astype(F32)
            for at in range(4):
                @pl.when(y == at)
                def _(at=at):
                    cols = slice(at * PANEL, (at + 1) * PANEL)
                    acc[:, cols] = acc[:, cols] + extra
            rows = lax.broadcasted_iota(jnp.int32, (128, K), 0)
            cols = lax.broadcasted_iota(jnp.int32, (128, K), 1)
            acc[...] = acc[...] - jnp.where(cols == rows + place * 128, SHIFT, 0.0)

    final = acc[...].astype(BF16)
    for peer in range(8):
        out[peer] = final


def slab(scal, part, raws, us, vs, ks):
    args = list(raws) + [us] + list(vs) + list(ks)
    return simple(
        lambda *refs: slab_kernel(*refs, part=part), scal, args, [shape(8, 128, K)],
        scratch=[pltpu.VMEM((128, 512), BF16), pltpu.VMEM((K, 512), BF16), pltpu.VMEM((128, K), F32)],
        flops=2 * 128 * K * 512,
    )[0]


def assemble_kernel(scal, front, us, v0, v1, v2, v3, out, left, right):
    row = scal[0]
    step = pl.program_id(0)
    window, at = step // 4, step % 4

    @pl.when(step == 0)
    def _():
        for s, v in enumerate((v0, v1, v2, v3)):
            right[:, s * 128 : (s + 1) * 128] = v[...]

    for s in range(4):
        kid = (row - s) & 3
        hits = [spot(scal, kid, 2 * row + window, q) == at for q in range(4)]
        for half in range(2):
            value = chosen(hits, [us[2 * q + half, window, kid] for q in range(4)])
            left[half * 128 : (half + 1) * 128, s * 128 : (s + 1) * 128] = value.astype(BF16)
    out[...] = front[...] + lax.dot_general(
        left[...], right[...], (((1,), (1,)), ((), ())), preferred_element_type=F32
    )


def assemble(scal, front, us, vs):
    rows, cols = front.shape
    args = [front, us] + list(vs)
    block = pl.BlockSpec((PANEL, cols), lambda i, s: (i, 0))
    return call(
        assemble_kernel, scal, args,
        [block] + [whole(x.shape) for x in args[1:]],
        shape(rows, cols, dtype=F32), block, grid=(rows // PANEL,),
        scratch=[pltpu.VMEM((PANEL, 512), BF16), pltpu.VMEM((cols, 512), BF16)],
        flops=2 * rows * cols * 512,
    )


TALL = 2 * PANEL


def trail_kernel(scal, tile, kc, top, low, g0, g1, g2, g3, d0, d1, d2, d3, out):
    row, y, h, place = scal[0], scal[1], scal[2], scal[3]
    step = pl.program_id(0)
    gs = (g0, g1, g2, g3)

    @pl.when((row == 0) & (step < 2))
    def _():
        out[...] = kc[...]

    def update(rows):
        @pl.when(place == 0)
        def _():
            for q, g in enumerate(gs):
                out[:, q * PANEL : (q + 1) * PANEL] = dot(rows[...], g[...])

        @pl.when(place != 0)
        def _():
            for q, g in enumerate(gs):
                cols = slice(q * PANEL, (q + 1) * PANEL)
                out[:, cols] = tile[:, cols] - dot(rows[...], g[...])
            for s, d in enumerate((d0, d1, d2, d3)):
                for at in range(4):
                    @pl.when((row == y) & (step == 2 * h + at // 2) & (((row - s) & 3) == at))
                    def _(at=at, d=d):
                        rows_at = slice(at % 2 * PANEL, (at % 2 + 1) * PANEL)
                        cols = slice(at * PANEL, (at + 1) * PANEL)
                        out[rows_at, cols] = out[rows_at, cols] + d[...].astype(F32)

    @pl.when((row != 0) & (step < 2))
    def _():
        update(top)

    @pl.when(step >= 2)
    def _():
        update(low)


def trail(scal, tile, kc, top, low, gs, ds):
    rows, cols = tile.shape
    block = pl.BlockSpec((TALL, cols), lambda i, s: (i, 0))
    first = pl.BlockSpec((TALL, cols), lambda i, s: (jnp.minimum(i, 1), 0))
    second = pl.BlockSpec((TALL, cols), lambda i, s: (jnp.maximum(i, 2) - 2, 0))
    args = [tile, kc, top, low] + list(gs) + list(ds)
    return call(
        trail_kernel, scal, args,
        [block, first, first, second] + [whole(x.shape) for x in args[4:]],
        shape(rows, cols, dtype=F32), block, grid=(rows // TALL,),
        flops=2 * rows * cols * K,
    )


def spread(pieces, y):
    got = [pieces[0]] + [lax.ppermute(pieces[i], COL, [(0, 2 * i)]) for i in range(1, 4)]
    mine = total([y == i for i in range(4)], got)
    return mine, lax.ppermute(mine[128:], COL, [(2 * i, 2 * i + 1) for i in range(4)])


def over_rows(value):
    return [value] + [
        lax.ppermute(value, "row", [(i, (i + s) % 4) for i in range(4)]) for s in range(1, 4)
    ]


def after(value, token):
    return lax.optimization_barrier((value, token))[0]


def local(front_entries, kid_u, kid_v, kid_d, kid_counts, kid_blocks):
    children, _, rank = kid_u.shape
    f = lax.axis_index("front")
    r = lax.axis_index("row")
    y = lax.axis_index("col_0")
    h = lax.axis_index("col_1")
    place = 2 * y + h
    first_child = (f + 3) % 4 * children
    counts = lax.dynamic_slice_in_dim(kid_counts, first_child, children, 0)
    blocks = lax.dynamic_slice_in_dim(kid_blocks, first_child, children, 0)
    scal = jnp.concatenate((jnp.stack([r, y, h, place]), counts, blocks.reshape(-1))).astype(jnp.int32)
    front = front_entries[0]

    def moved(make):
        out = []
        for k in range(4):
            pairs = [(i * 4 + j, (i + 1) % 4 * 4 + (j + k) % 4) for i in range(4) for j in range(4)]
            out.append(lax.ppermute(make(k), ("front", "row"), pairs))
        return out

    got_p = moved(lambda k: lax.dynamic_index_in_dim(kid_v, (r + k) % 4, 0, keepdims=False))
    got_u = moved(lambda k: kid_u)
    got_d = moved(lambda k: kid_d)

    send = simple(pick_right_kernel, scal, got_p, [shape(8, 128, 256)])[0]
    back_v = lax.all_to_all(send, COL, 0, 0)
    slots = simple(pick_left_kernel, scal, got_u, [shape(8, 2, 4, 128, rank)])[0]
    all_u = lax.all_to_all(after(slots, back_v[0, 0, 0]), COL, 0, 0)
    raw_top = spread(halve(scal, front, 0), y)
    raw_low = spread(halve(scal, front, 1), y)
    send = simple(pick_blocks_kernel, scal, got_d, [shape(8, 128, PANEL)])[0]
    back_d = lax.all_to_all(after(send, all_u[0, 0, 0, 0, 0]), COL, 0, 0)
    v_own, v_first = simple(place_right_kernel, scal, [back_v], [shape(K, rank), shape(K, rank)])
    vs_first = over_rows(v_first)
    d_mine = simple(place_blocks_kernel, scal, [back_d], [shape(PANEL, PANEL)])[0]
    ks = [
        lax.ppermute(d_mine[half * 128 : (half + 1) * 128], ROW_COL, [(8 * p, 2 * p + half) for p in range(4)])
        for half in range(2)
    ]
    slab_top = slab(scal, 0, raw_top, all_u, vs_first, ks)
    top = lax.all_to_all(slab_top, COL, 0, 0).reshape(K, K)
    token = slab_top[0, 0, 0]
    slab_low = slab(scal, 1, raw_low, all_u, vs_first, ())
    vs = over_rows(after(v_own, token))
    ds = [d_mine]
    for s in range(1, 4):
        pairs = [
            (((t - s) % 4) * 8 + 2 * t + x, t * 8 + 2 * t + x) for t in range(4) for x in range(2)
        ]
        ds.append(lax.ppermute(after(d_mine, token), ROW_COL, pairs))
    tile = assemble(scal, front, all_u, vs)
    kc, *g = factor(scal, tile, top)
    low = lax.all_to_all(after(slab_low, kc[0, 0]), COL, 0, 0).reshape(K, K)

    def up(value, hops):
        return lax.ppermute(value, "row", [(i, i + 1) for i in range(hops)])

    def down(value, hops):
        return lax.ppermute(value, "row", [(-i % 4, -(i + 1) % 4) for i in range(hops)])

    root = r == 0
    up1, down1 = lax.optimization_barrier((up(g[0], 1), down(g[3], 1)))
    pair = lax.optimization_barrier((jnp.where(root, g[1], up1), jnp.where(root, g[2], down1)))
    up2, down2 = lax.optimization_barrier((up(pair[0], 2), down(pair[1], 2)))
    pair = lax.optimization_barrier((jnp.where(root, g[2], up2), jnp.where(root, g[1], down2)))
    up3, down3 = up(pair[0], 3), down(pair[1], 3)
    rows_are = [r == i for i in range(4)]
    quarters = [
        total(rows_are, (g[0], up1, up2, up3)),
        total(rows_are, (g[1], up2, up3, down3)),
        total(rows_are, (g[2], up3, down3, down2)),
        total(rows_are, (g[3], down3, down2, down1)),
    ]
    return trail(scal, tile, kc, top, low, quarters, ds)[None]


def solution(mesh):
    finer = Mesh(
        mesh.devices.reshape(mesh.shape["front"], mesh.shape["row"], 4, 2),
        ("front", "row", "col_0", "col_1"),
    )
    in_specs = (
        P("front", "row", COL),
        P("front", ROW_COL, None),
        P("front", ROW_COL, None),
        P("front", ROW_COL, None),
        P(),
        P(),
    )
    out_specs = P("front", "row", COL)
    return jax.shard_map(local, mesh=finer, in_specs=in_specs, out_specs=out_specs, check_vma=False)
```

```python
import jax
import jax.numpy as jnp
from jax import lax
from jax.experimental import pallas as pl
from jax.experimental.pallas import tpu as pltpu
from jax.sharding import Mesh
from jax.sharding import PartitionSpec as P


PANEL = 256
PANELS = 4
K = PANEL * PANELS
COL = ("col_0", "col_1")
ROW_COL = ("row", "col_0", "col_1")
F32 = jnp.float32
BF16 = jnp.bfloat16


def dot(a, b):
    return jnp.dot(a, b, preferred_element_type=F32)


def split(a):
    high = a.astype(BF16)
    return high, (a - high.astype(F32)).astype(BF16)


def total(flags, values):
    out = None
    for flag, value in zip(flags, values):
        piece = jnp.where(flag, value, jnp.zeros_like(value))
        out = piece if out is None else out + piece
    return out


SHIFT = 96.0


def identity():
    rows = lax.broadcasted_iota(jnp.int32, (PANEL, PANEL), 0)
    return rows == lax.broadcasted_iota(jnp.int32, (PANEL, PANEL), 1)


def invert_into(inv, index, pivot):
    eye = identity()
    one = jnp.where(eye, 1.0, 0.0)
    diagonal = jnp.where(eye, pivot, 0.0)
    down = 1.0 / jnp.sum(diagonal, axis=1, keepdims=True)
    across = 1.0 / jnp.sum(diagonal, axis=0, keepdims=True)
    rest = jnp.where(eye, 0.0, -pivot * across)
    power = rest.astype(BF16)
    series = one + rest
    for _ in range(3):
        power = dot(power, power).astype(BF16)
        series = series + dot(series.astype(BF16), power)
    inv[index] = series * down
    p_high, p_low = split(pivot)

    def improve():
        x = inv[index]
        x_high, x_low = split(x)
        error = one - (dot(p_high, x_high) + (dot(p_high, x_low) + dot(p_low, x_high)))
        inv[index] = x + dot(x_high, error.astype(BF16))
        square = error * error
        return jnp.max(jnp.sum(square, axis=0)) * jnp.max(jnp.sum(square, axis=1))

    size = improve()

    @pl.when(jnp.logical_not(size < 0.5))
    def _():
        norm = jnp.max(jnp.sum(jnp.abs(pivot), axis=0)) * jnp.max(jnp.sum(jnp.abs(pivot), axis=1))
        inv[index] = pivot.T * (1.0 / norm)

    def more(carry):
        trips, _ = carry
        return trips + 1, improve()

    lax.while_loop(
        lambda carry: (carry[0] < 100) & jnp.logical_not(carry[1] < 4e-6), more, (jnp.int32(0), size)
    )


def factor_kernel(scal, tile, top, kc, g0, g1, g2, g3, a, c, inv):
    outs = (g0, g1, g2, g3)
    row, place = scal[0], scal[3]

    @pl.when(row == 0)
    def _():
        a[...] = top[...].astype(F32)
        for k in range(PANELS):
            s, e = k * PANEL, (k + 1) * PANEL
            a[s:e, s:e] = a[s:e, s:e] + jnp.where(identity(), SHIFT, 0.0)

        @pl.when(place == 0)
        def _():
            c[...] = a[...]

        @pl.when(place != 0)
        def _():
            c[...] = tile[...]

        for k in range(PANELS):
            s, e = k * PANEL, (k + 1) * PANEL
            invert_into(inv, k, a[s:e, s:e])
            if e < K:
                lower = dot(a[e:, s:e].astype(BF16), inv[k].astype(BF16))
                a[e:, s:e] = lower
                lower_b = lower.astype(BF16)
                a[e:, e:] = a[e:, e:] - dot(lower_b, a[s:e, e:].astype(BF16))
                c[e:, :] = c[e:, :] - dot(lower_b, c[s:e, :].astype(BF16))

        @pl.when(place == 0)
        def _():
            kc[...] = a[...]
            rows = lax.broadcasted_iota(jnp.int32, (K, K), 0)
            cols = lax.broadcasted_iota(jnp.int32, (K, K), 1)
            c[...] = jnp.where(rows == cols, 1.0, 0.0)

        @pl.when(place != 0)
        def _():
            kc[...] = c[...]

        for k in reversed(range(PANELS)):
            s, e = k * PANEL, (k + 1) * PANEL
            part = dot(inv[k].astype(BF16), c[s:e, :].astype(BF16))
            part_b = part.astype(BF16)
            for q in range(4):
                outs[q][s:e, :] = part_b[:, q * PANEL : (q + 1) * PANEL]
            if k:
                c[:s, :] = c[:s, :] - dot(a[:s, s:e].astype(BF16), part_b)


def whole(shape):
    return pl.BlockSpec(shape, lambda i, s: (0,) * len(shape))


def call(kernel, scal, args, in_specs, outs, out_specs, grid=(1,), scratch=(), flops=0):
    moved = sum(x.size * x.dtype.itemsize for x in args)
    single = not isinstance(outs, tuple)
    return pl.pallas_call(
        kernel,
        out_shape=outs,
        grid_spec=pltpu.PrefetchScalarGridSpec(
            num_scalar_prefetch=1,
            grid=grid,
            in_specs=in_specs,
            out_specs=out_specs if single else tuple(out_specs),
            scratch_shapes=list(scratch),
        ),
        compiler_params=pltpu.CompilerParams(vmem_limit_bytes=56 * 1024 * 1024),
        cost_estimate=pl.CostEstimate(flops=flops, bytes_accessed=2 * moved, transcendentals=0),
    )(scal, *args)


def simple(kernel, scal, args, outs, scratch=(), flops=0):
    return call(
        kernel, scal, args, [whole(x.shape) for x in args], tuple(outs),
        [whole(x.shape) for x in outs], scratch=scratch, flops=flops,
    )


def shape(*dims, dtype=BF16):
    return jax.ShapeDtypeStruct(dims, dtype)


def factor(scal, tile, top):
    return call(
        factor_kernel, scal, [tile, top],
        [whole((K, K)), whole((K, K))],
        (shape(K, K, dtype=F32),) + (shape(K, PANEL),) * 4,
        [whole((K, K))] + [whole((K, PANEL))] * 4,
        scratch=[pltpu.VMEM((K, K), F32), pltpu.VMEM((K, K), F32), pltpu.VMEM((PANELS, PANEL, PANEL), F32)],
        flops=10 * K * K * K,
    )


COUNT_AT, BLOCK_AT = 4, 8


def block_of(scal, kid, source_row, q):
    return scal[BLOCK_AT + kid * 16 + source_row * 4 + q]


def spot(scal, kid, window, q):
    at = jnp.int32(-1)
    for source_row in range(4):
        block = block_of(scal, kid, source_row, q)
        at = jnp.where((block >> 2) == window, block & 3, at)
    return at


def chosen(flags, values):
    acc = None
    for flag, value in zip(flags, values):
        value = value.astype(F32)
        value = jnp.where(flag, value, jnp.zeros_like(value))
        acc = value if acc is None else acc + value
    return acc


def halve_kernel(scal, front, *outs):
    for i, out in enumerate(outs):
        out[...] = front[i * PANEL : (i + 1) * PANEL, :].astype(BF16)


def halve(scal, front, part):
    return call(
        halve_kernel, scal, [front], [pl.BlockSpec((K, K), lambda i, s: (part, 0))],
        (shape(PANEL, K),) * 4, [whole((PANEL, K))] * 4,
    )


def pick_left_kernel(scal, u0, u1, u2, u3, out):
    row, y = scal[0], scal[1]
    lane = lax.broadcasted_iota(jnp.int32, (128, 128), 1)
    for kid in range(4):
        live = lane < scal[COUNT_AT + kid]
        blocks = [block_of(scal, kid, (row - k) & 3, y) for k in range(4)]
        for window in range(2):
            flags = [(b >> 2) == 2 * row + window for b in blocks]
            value = chosen(flags, [u[kid] for u in (u0, u1, u2, u3)])
            value = jnp.where(live, value, 0.0).astype(BF16)
            for peer in range(8):
                out[peer, window, kid] = value


def pick_right_kernel(scal, p0, p1, p2, p3, out):
    row, y = scal[0], scal[1]
    blocks = [block_of(scal, row, (row - k) & 3, y) for k in range(4)]
    rights = [p[...] for p in (p0, p1, p2, p3)]
    first = chosen([(b >> 2) == 0 for b in blocks], rights).astype(BF16)
    for peer in range(8):
        out[peer, :, :128] = chosen([(b >> 2) == peer for b in blocks], rights).astype(BF16)
        out[peer, :, 128:] = first


def pick_blocks_kernel(scal, d0, d1, d2, d3, out):
    row, y = scal[0], scal[1]
    for window in range(8):
        flags, values = [], []
        for kid in range(4):
            for k, d in enumerate((d0, d1, d2, d3)):
                flags.append(block_of(scal, kid, (row - k) & 3, y) == 4 * window + row)
                values.append(d[kid])
        out[window] = chosen(flags, values).astype(BF16)


def place_right_kernel(scal, back, out_own, out_first):
    row, place = scal[0], scal[3]
    own = [spot(scal, row, place, q) for q in range(4)]
    first = [spot(scal, row, 0, q) for q in range(4)]
    for at in range(4):
        for half in range(2):
            rows = slice((2 * at + half) * 128, (2 * at + half + 1) * 128)
            for spots, out, cols in ((own, out_own, slice(0, 128)), (first, out_first, slice(128, 256))):
                flags = [spots[q] == at for q in range(4)]
                out[rows, :] = chosen(flags, [back[2 * q + half, :, cols] for q in range(4)]).astype(BF16)


def place_blocks_kernel(scal, back, out):
    for half in range(2):
        acc = back[half].astype(F32)
        for q in range(1, 4):
            acc = acc + back[2 * q + half].astype(F32)
        out[half * 128 : (half + 1) * 128, :] = acc.astype(BF16)


def slab_kernel(scal, near, far, us, *refs, part):
    vs, ks = refs[:4], refs[4:-4]
    out, left, right, acc = refs[-4:]
    row, y, h, place = scal[0], scal[1], scal[2], scal[3]
    for s in range(4):
        kid = (row - s) & 3
        right[:, s * 128 : (s + 1) * 128] = vs[s][...]
        hits = [spot(scal, kid, 2 * row + part, q) == y for q in range(4)]
        value = chosen(hits, [us[2 * q + h, part, kid] for q in range(4)])
        left[:, s * 128 : (s + 1) * 128] = value.astype(BF16)
    raw = jnp.where(h == 0, near[:128, :].astype(F32), far[...].astype(F32))
    acc[...] = raw + lax.dot_general(
        left[...], right[...], (((1,), (1,)), ((), ())), preferred_element_type=F32
    )
    if ks:
        @pl.when(row == 0)
        def _():
            extra = ks[0][...].astype(F32) + ks[1][...].astype(F32)
            for at in range(4):
                @pl.when(y == at)
                def _(at=at):
                    cols = slice(at * PANEL, (at + 1) * PANEL)
                    acc[:, cols] = acc[:, cols] + extra
            rows = lax.broadcasted_iota(jnp.int32, (128, K), 0)
            cols = lax.broadcasted_iota(jnp.int32, (128, K), 1)
            acc[...] = acc[...] - jnp.where(cols == rows + place * 128, SHIFT, 0.0)

    final = acc[...].astype(BF16)
    for peer in range(8):
        out[peer] = final


def slab(scal, part, raws, us, vs, ks):
    args = list(raws) + [us] + list(vs) + list(ks)
    return simple(
        lambda *refs: slab_kernel(*refs, part=part), scal, args, [shape(8, 128, K)],
        scratch=[pltpu.VMEM((128, 512), BF16), pltpu.VMEM((K, 512), BF16), pltpu.VMEM((128, K), F32)],
        flops=2 * 128 * K * 512,
    )[0]


def assemble_kernel(scal, front, us, v0, v1, v2, v3, out, left, right):
    row = scal[0]
    step = pl.program_id(0)
    window, at = step // 4, step % 4

    @pl.when(step == 0)
    def _():
        for s, v in enumerate((v0, v1, v2, v3)):
            right[:, s * 128 : (s + 1) * 128] = v[...]

    for s in range(4):
        kid = (row - s) & 3
        hits = [spot(scal, kid, 2 * row + window, q) == at for q in range(4)]
        for half in range(2):
            value = chosen(hits, [us[2 * q + half, window, kid] for q in range(4)])
            left[half * 128 : (half + 1) * 128, s * 128 : (s + 1) * 128] = value.astype(BF16)
    out[...] = front[...] + lax.dot_general(
        left[...], right[...], (((1,), (1,)), ((), ())), preferred_element_type=F32
    )


def assemble(scal, front, us, vs):
    rows, cols = front.shape
    args = [front, us] + list(vs)
    block = pl.BlockSpec((PANEL, cols), lambda i, s: (i, 0))
    return call(
        assemble_kernel, scal, args,
        [block] + [whole(x.shape) for x in args[1:]],
        shape(rows, cols, dtype=F32), block, grid=(rows // PANEL,),
        scratch=[pltpu.VMEM((PANEL, 512), BF16), pltpu.VMEM((cols, 512), BF16)],
        flops=2 * rows * cols * 512,
    )


TALL = 2 * PANEL


def trail_kernel(scal, tile, kc, top, low, g0, g1, g2, g3, d0, d1, d2, d3, out):
    row, y, h, place = scal[0], scal[1], scal[2], scal[3]
    step = pl.program_id(0)
    gs = (g0, g1, g2, g3)

    @pl.when((row == 0) & (step < 2))
    def _():
        out[...] = kc[...]

    def update(rows):
        @pl.when(place == 0)
        def _():
            for q, g in enumerate(gs):
                out[:, q * PANEL : (q + 1) * PANEL] = dot(rows[...], g[...])

        @pl.when(place != 0)
        def _():
            for q, g in enumerate(gs):
                cols = slice(q * PANEL, (q + 1) * PANEL)
                out[:, cols] = tile[:, cols] - dot(rows[...], g[...])
            for s, d in enumerate((d0, d1, d2, d3)):
                for at in range(4):
                    @pl.when((row == y) & (step == 2 * h + at // 2) & (((row - s) & 3) == at))
                    def _(at=at, d=d):
                        rows_at = slice(at % 2 * PANEL, (at % 2 + 1) * PANEL)
                        cols = slice(at * PANEL, (at + 1) * PANEL)
                        out[rows_at, cols] = out[rows_at, cols] + d[...].astype(F32)

    @pl.when((row != 0) & (step < 2))
    def _():
        update(top)

    @pl.when(step >= 2)
    def _():
        update(low)


def trail(scal, tile, kc, top, low, gs, ds):
    rows, cols = tile.shape
    block = pl.BlockSpec((TALL, cols), lambda i, s: (i, 0))
    first = pl.BlockSpec((TALL, cols), lambda i, s: (jnp.minimum(i, 1), 0))
    solved = pl.BlockSpec((TALL, cols), lambda i, s: (jnp.where(s[0] == 0, jnp.minimum(i, 1), 0), 0))
    tiles = pl.BlockSpec((TALL, cols), lambda i, s: (jnp.where(s[0] == 0, jnp.maximum(i, 2), i), 0))
    second = pl.BlockSpec((TALL, cols), lambda i, s: (jnp.maximum(i, 2) - 2, 0))
    args = [tile, kc, top, low] + list(gs) + list(ds)
    return call(
        trail_kernel, scal, args,
        [tiles, solved, first, second] + [whole(x.shape) for x in args[4:]],
        shape(rows, cols, dtype=F32), block, grid=(rows // TALL,),
        flops=2 * rows * cols * K,
    )


def spread(pieces, y):
    got = [pieces[0]] + [lax.ppermute(pieces[i], COL, [(0, 2 * i)]) for i in range(1, 4)]
    mine = total([y == i for i in range(4)], got)
    return mine, lax.ppermute(mine[128:], COL, [(2 * i, 2 * i + 1) for i in range(4)])


def over_rows(value):
    return [value] + [
        lax.ppermute(value, "row", [(i, (i + s) % 4) for i in range(4)]) for s in range(1, 4)
    ]


def after(value, token):
    return lax.optimization_barrier((value, token))[0]


def local(front_entries, kid_u, kid_v, kid_d, kid_counts, kid_blocks):
    children, _, rank = kid_u.shape
    f = lax.axis_index("front")
    r = lax.axis_index("row")
    y = lax.axis_index("col_0")
    h = lax.axis_index("col_1")
    place = 2 * y + h
    first_child = (f + 3) % 4 * children
    counts = lax.dynamic_slice_in_dim(kid_counts, first_child, children, 0)
    blocks = lax.dynamic_slice_in_dim(kid_blocks, first_child, children, 0)
    scal = jnp.concatenate((jnp.stack([r, y, h, place]), counts, blocks.reshape(-1))).astype(jnp.int32)
    front = front_entries[0]

    def moved(make):
        out = []
        for k in range(4):
            pairs = [(i * 4 + j, (i + 1) % 4 * 4 + (j + k) % 4) for i in range(4) for j in range(4)]
            out.append(lax.ppermute(make(k), ("front", "row"), pairs))
        return out

    got_p = moved(lambda k: lax.dynamic_index_in_dim(kid_v, (r + k) % 4, 0, keepdims=False))
    got_u = moved(lambda k: kid_u)
    got_d = moved(lambda k: kid_d)

    send = simple(pick_right_kernel, scal, got_p, [shape(8, 128, 256)])[0]
    back_v = lax.all_to_all(send, COL, 0, 0)
    slots = simple(pick_left_kernel, scal, got_u, [shape(8, 2, 4, 128, rank)])[0]
    all_u = lax.all_to_all(after(slots, back_v[0, 0, 0]), COL, 0, 0)
    raw_top = spread(halve(scal, front, 0), y)
    low_pieces = halve(scal, front, 1)
    raw_low = spread(low_pieces, y)
    send = simple(pick_blocks_kernel, scal, got_d, [shape(8, 128, PANEL)])[0]
    back_d = lax.all_to_all(after(send, all_u[0, 0, 0, 0, 0]), COL, 0, 0)
    v_own, v_first = simple(place_right_kernel, scal, [back_v], [shape(K, rank), shape(K, rank)])
    vs_first = over_rows(v_first)
    d_mine = simple(place_blocks_kernel, scal, [back_d], [shape(PANEL, PANEL)])[0]
    ks = [
        lax.ppermute(d_mine[half * 128 : (half + 1) * 128], ROW_COL, [(8 * p, 2 * p + half) for p in range(4)])
        for half in range(2)
    ]
    slab_top = slab(scal, 0, raw_top, all_u, vs_first, ks)
    top = lax.all_to_all(slab_top, COL, 0, 0).reshape(K, K)
    token = slab_top[0, 0, 0]
    slab_low = slab(scal, 1, raw_low, all_u, vs_first, ())
    vs = over_rows(v_own)
    ds = [d_mine]
    for s in range(1, 4):
        pairs = [
            (((t - s) % 4) * 8 + 2 * t + x, t * 8 + 2 * t + x) for t in range(4) for x in range(2)
        ]
        ds.append(lax.ppermute(after(d_mine, token), ROW_COL, pairs))
    tile = assemble(scal, front, all_u, vs)
    kc, *g = factor(scal, tile, top)
    low = lax.all_to_all(after(slab_low, kc[0, 0]), COL, 0, 0).reshape(K, K)

    def up(value, hops):
        return lax.ppermute(value, "row", [(i, i + 1) for i in range(hops)])

    def down(value, hops):
        return lax.ppermute(value, "row", [(-i % 4, -(i + 1) % 4) for i in range(hops)])

    root = r == 0
    up1, down1 = lax.optimization_barrier((up(g[0], 1), down(g[3], 1)))
    pair = lax.optimization_barrier((jnp.where(root, g[1], up1), jnp.where(root, g[2], down1)))
    up2, down2 = lax.optimization_barrier((up(pair[0], 2), down(pair[1], 2)))
    pair = lax.optimization_barrier((jnp.where(root, g[2], up2), jnp.where(root, g[1], down2)))
    up3, down3 = up(pair[0], 3), down(pair[1], 3)
    rows_are = [r == i for i in range(4)]
    quarters = [
        total(rows_are, (g[0], up1, up2, up3)),
        total(rows_are, (g[1], up2, up3, down3)),
        total(rows_are, (g[2], up3, down3, down2)),
        total(rows_are, (g[3], down3, down2, down1)),
    ]
    return trail(scal, tile, kc, top, low, quarters, ds)[None]


def solution(mesh):
    finer = Mesh(
        mesh.devices.reshape(mesh.shape["front"], mesh.shape["row"], 4, 2),
        ("front", "row", "col_0", "col_1"),
    )
    in_specs = (
        P("front", "row", COL),
        P("front", ROW_COL, None),
        P("front", ROW_COL, None),
        P("front", ROW_COL, None),
        P(),
        P(),
    )
    out_specs = P("front", "row", COL)
    return jax.shard_map(local, mesh=finer, in_specs=in_specs, out_specs=out_specs, check_vma=False)
```
